32 devices in a mesh: dp: 1 (over z), sp: 4 (over y), cp: 8 (over x, core).
Axes of the slice: x: 4, y: 4, z: 1, core: 2. Of those that a mesh axis runs over, the one named last changes fastest.
The devices are a block of a 4x4x8 slice.
Arguments:
- x_chunk: bfloat16 [4096, 5120], P(('dp', 'sp', 'cp'))
- k_cache: bfloat16 [4096, 40, 128], P(('dp', 'sp', 'cp'))
- v_cache: bfloat16 [4096, 40, 128], P(('dp', 'sp', 'cp'))
- w_q: bfloat16 [5120, 5120], replicated
- w_k: bfloat16 [5120, 5120], replicated
- w_v: bfloat16 [5120, 5120], replicated
- w_o: bfloat16 [5120, 5120], replicated
Outputs:
- output 1: bfloat16 [4096, 5120], P(('dp', 'sp', 'cp'))
- output 2: bfloat16 [4096, 40, 128], P(('dp', 'sp', 'cp'))
- output 3: bfloat16 [4096, 40, 128], P(('dp', 'sp', 'cp'))
All inputs are finite; a program needn't handle non-finite values.
Results may differ from the reference program's by a relative error of at most 0.00540798.
Values are sent between devices in bfloat16 or wider.
A program may use at most 768 MiB of HBM per device.

```python
import math
import jax
import jax.numpy as jnp
from jax import lax

D_MODEL = 5120
HEADS = 40
KV_HEADS = 40
HEAD = 128
TOK = 4096
CACHE = 4096
SHARDS = 32
QBLOCK = 16
ROPE_BASE = 500000


def rope_tables(positions):
    inv_freq = 1.0 / (ROPE_BASE ** (jnp.arange(0, HEAD, 2, dtype=jnp.float32) / HEAD))
    angles = positions.astype(jnp.float32)[:, None] * inv_freq[None, :]
    return jnp.cos(angles), jnp.sin(angles)


def apply_rope(values, cos_t, sin_t):
    half_dim = HEAD // 2
    lo_half = values[..., :half_dim].astype(jnp.float32)
    hi_half = values[..., half_dim:].astype(jnp.float32)
    return jnp.concatenate([lo_half * cos_t - hi_half * sin_t, hi_half * cos_t + lo_half * sin_t], axis=-1).astype(jnp.bfloat16)


def setup_inputs(seed: int = 0, part: int = 0) -> dict:
    group_size = HEADS // KV_HEADS
    shard_len = CACHE // SHARDS
    score_gap = max(1.0, math.log(CACHE / TOK) + 1.0)
    shared_keys = jax.random.split(jax.random.key(seed), 7)
    part_keys = jax.random.split(jax.random.fold_in(jax.random.key(seed + 1), part), 5)
    x_mean = 0.6 * jax.random.normal(shared_keys[0], (D_MODEL,), jnp.float32)
    low_dims = (jnp.arange(HEAD) % (HEAD // 2)) >= (HEAD // 2 - 8)
    bias_dir = jax.random.normal(shared_keys[1], (KV_HEADS, HEAD), jnp.float32) * low_dims
    bias_kv = bias_dir / jnp.linalg.norm(bias_dir, axis=-1, keepdims=True) * math.sqrt(score_gap * math.sqrt(HEAD))
    bias_q = jnp.repeat(bias_kv, group_size, axis=0).reshape(HEADS * HEAD)
    mean_lift = x_mean[:, None] / jnp.sum(x_mean * x_mean)
    w_q = jax.random.normal(shared_keys[2], (D_MODEL, HEADS * HEAD), jnp.float32) * D_MODEL ** -0.5 + mean_lift * bias_q[None, :]
    w_k = jax.random.normal(shared_keys[3], (D_MODEL, KV_HEADS * HEAD), jnp.float32) * D_MODEL ** -0.5 + mean_lift * bias_kv.reshape(KV_HEADS * HEAD)[None, :]
    w_v = jax.random.normal(shared_keys[4], (D_MODEL, KV_HEADS * HEAD), jnp.float32) * D_MODEL ** -0.5
    w_o = jax.random.normal(shared_keys[5], (HEADS * HEAD, D_MODEL), jnp.float32) * (HEADS * HEAD) ** -0.5
    x_chunk = 0.8 * jax.random.normal(part_keys[0], (TOK, D_MODEL), jnp.float32) + x_mean[None, :]
    key_scale = jnp.exp(jax.random.uniform(part_keys[1], (SHARDS, 1, 1, 1), jnp.float32, -0.7, 0.7)) / math.sqrt(1.0 + score_gap / math.sqrt(HEAD))
    k_cache = (jax.random.normal(part_keys[2], (SHARDS, shard_len, KV_HEADS, HEAD), jnp.float32) * key_scale).reshape(CACHE, KV_HEADS, HEAD)
    val_mean = jax.random.normal(part_keys[3], (SHARDS, 1, KV_HEADS, HEAD), jnp.float32)
    v_cache = (0.5 * jax.random.normal(part_keys[4], (SHARDS, shard_len, KV_HEADS, HEAD), jnp.float32) + val_mean).reshape(CACHE, KV_HEADS, HEAD)
    return {'x_chunk': x_chunk.astype(jnp.bfloat16), 'k_cache': k_cache.astype(jnp.bfloat16), 'v_cache': v_cache.astype(jnp.bfloat16), 'w_q': w_q.astype(jnp.bfloat16), 'w_k': w_k.astype(jnp.bfloat16), 'w_v': w_v.astype(jnp.bfloat16), 'w_o': w_o.astype(jnp.bfloat16)}


def reference(x_chunk, k_cache, v_cache, w_q, w_k, w_v, w_o):
    group_size = HEADS // KV_HEADS
    attn_scale = HEAD ** -0.5
    cos_t, sin_t = rope_tables(CACHE + jnp.arange(TOK))
    q_rows = jnp.dot(x_chunk, w_q, preferred_element_type=jnp.float32).astype(jnp.bfloat16)
    q_heads = apply_rope(q_rows.reshape(TOK, KV_HEADS, group_size, HEAD), cos_t[:, None, None, :], sin_t[:, None, None, :])
    k_rows = jnp.dot(x_chunk, w_k, preferred_element_type=jnp.float32).astype(jnp.bfloat16)
    k_new = apply_rope(k_rows.reshape(TOK, KV_HEADS, HEAD), cos_t[:, None, :], sin_t[:, None, :])
    v_new = jnp.dot(x_chunk, w_v, preferred_element_type=jnp.float32).astype(jnp.bfloat16).reshape(TOK, KV_HEADS, HEAD)
    keys_all = jnp.concatenate([k_cache, k_new], axis=0)
    vals_all = jnp.concatenate([v_cache, v_new], axis=0)
    key_pos = jnp.arange(CACHE + TOK)
    block_starts = jnp.arange(TOK // QBLOCK) * QBLOCK

    def per_head(head_args):
        q_head, k_head, v_head = head_args
        k_trans = k_head.T

        def per_block(block_args):
            q_block, row_start = block_args
            scores = jnp.dot(q_block.reshape(QBLOCK * group_size, HEAD), k_trans, preferred_element_type=jnp.float32)
            scores = scores.reshape(QBLOCK, group_size, CACHE + TOK) * attn_scale
            allowed = key_pos[None, None, :] <= (CACHE + row_start + jnp.arange(QBLOCK))[:, None, None]
            scores = jnp.where(allowed, scores, -jnp.inf)
            row_max = jnp.max(scores, axis=-1, keepdims=True)
            exp_scores = jnp.exp(scores - row_max)
            row_sum = jnp.sum(exp_scores, axis=-1, keepdims=True)
            out_block = jnp.dot(exp_scores.astype(jnp.bfloat16).reshape(QBLOCK * group_size, CACHE + TOK), v_head, preferred_element_type=jnp.float32)
            return out_block.reshape(QBLOCK, group_size, HEAD) / row_sum

        blocks = lax.map(per_block, (q_head.reshape(TOK // QBLOCK, QBLOCK, group_size, HEAD), block_starts))
        return blocks.reshape(TOK, group_size, HEAD)

    attn_out = lax.map(per_head, (jnp.transpose(q_heads, (1, 0, 2, 3)), jnp.transpose(keys_all, (1, 0, 2)), jnp.transpose(vals_all, (1, 0, 2))))
    attn_rows = jnp.transpose(attn_out, (1, 0, 2, 3)).reshape(TOK, HEADS * HEAD).astype(jnp.bfloat16)
    y_out = jnp.dot(attn_rows, w_o, preferred_element_type=jnp.float32).astype(jnp.bfloat16)
    return (y_out, k_new, v_new)
```

```python
import functools
import math

import jax
import jax.numpy as jnp
from jax import lax
from jax.experimental import pallas as pl
from jax.experimental.pallas import tpu as pltpu
from jax.sharding import PartitionSpec as P

ROPE_BASE = 500000
MESH = pl.DeviceIdType.MESH
COLS = 512
NBUF = 4
QB = 512
QC = QB // 2
KB = 1024


def rope_tables(positions, head_dim):
    inv_freq = 1.0 / (ROPE_BASE ** (jnp.arange(0, head_dim, 2, dtype=jnp.float32) / head_dim))
    angles = positions.astype(jnp.float32)[:, None] * inv_freq[None, :]
    cos_t, sin_t = jnp.cos(angles), jnp.sin(angles)
    return jnp.concatenate([cos_t, cos_t], axis=-1), jnp.concatenate([-sin_t, sin_t], axis=-1)


def online_step(q, k, v, m, l, acc, coef, mask=None):
    s = lax.dot_general(q, k, (((1,), (1,)), ((), ())), preferred_element_type=jnp.float32)
    if mask is not None:
        s = jnp.where(mask, s, -jnp.inf)
    m_new = jnp.maximum(m, jnp.max(s, axis=1, keepdims=True))
    p = jnp.exp2((s - m_new) * coef)
    alpha = jnp.exp2((m - m_new) * coef)
    part = p[:, :128]
    for lane in range(128, p.shape[1], 128):
        part = part + p[:, lane:lane + 128]
    pv = jnp.dot(p.astype(jnp.bfloat16), v, preferred_element_type=jnp.float32)
    return m_new, l * alpha + part, acc * alpha + pv


def kernel(sp, cp, heads, head_dim,
           x_ref, cos_ref, sin_ref, kc_hbm, vc_hbm, wq_hbm, wk_hbm, wv_hbm, wo_hbm,
           y_ref, kn_ref, vn_ref,
           q_loc, q_all, kc_all, vc_all, kn_all, vn_all, o_all, o_loc,
           m_st, l_st, acc_st, wbuf, wsem, ssem, rsem):
    S = sp * cp
    E = heads - S
    G = S // E
    t = x_ref.shape[0]
    d_model = x_ref.shape[1]
    L = S * t
    me = lax.axis_index('sp') * cp + lax.axis_index('cp')
    per = S // (2 * G)
    rank = lax.rem(me, G)
    xhead = S + lax.div(me, G)
    my_blk = lax.div(me, per)
    my_rank = jnp.minimum(my_blk, 2 * G - 1 - my_blk)
    hi_share = my_blk >= G
    own_extra = my_rank == rank
    coef = (head_dim ** -0.5) * math.log2(math.e)

    def dev(idx):
        return {'sp': lax.div(idx, cp), 'cp': lax.rem(idx, cp)}

    def col(h):
        return pl.ds(pl.multiple_of(h * head_dim, head_dim), head_dim)

    def rows(start, size):
        return pl.ds(pl.multiple_of(start, 128), size)

    def send(src, dst, sem, tgt):
        pltpu.make_async_remote_copy(src_ref=src, dst_ref=dst, send_sem=ssem.at[sem], recv_sem=rsem.at[sem],
                                     device_id=dev(tgt), device_id_type=MESH).start()

    def local(src, dst, sem):
        pltpu.make_async_copy(src, dst, rsem.at[sem]).start()

    def wait_recv(buf, sem):
        pltpu.make_async_copy(buf, buf, rsem.at[sem]).wait()

    def wait_sent(buf, n_pieces, sem):
        part = buf.at[pl.ds(0, n_pieces * t)]
        pltpu.make_async_copy(part, part, ssem.at[sem]).wait()

    tiles = d_model // COLS
    weights = (wq_hbm, wk_hbm, wv_hbm, wo_hbm)

    def fetch(w, tile, slot):
        return pltpu.make_async_copy(w.at[:, pl.ds(pl.multiple_of(tile * COLS, COLS), COLS)], wbuf.at[slot], wsem.at[slot])

    for tile in range(NBUF - 1):
        fetch(wq_hbm, tile, tile).start()

    barrier = pltpu.get_barrier_semaphore()

    def greet(d, carry):
        pl.semaphore_signal(barrier, inc=1, device_id=dev(lax.rem(me + d, S)), device_id_type=MESH)
        return carry

    lax.fori_loop(1, S, greet, 0)
    pl.semaphore_wait(barrier, S - 1)

    def send_kv(src, dst, sem):
        local(src.at[:, col(me)], dst.at[rows(me * t, t)], sem)
        local(src.at[:, col(xhead)], dst.at[rows(L + me * t, t)], sem)

    def send_pair(pair):
        for src, dst, sem in pair:
            send_kv(src, dst, sem)

        def to_peer(d, carry):
            tgt = lax.rem(me + d, S)
            for src, dst, sem in pair:
                send(src.at[:, col(tgt)], dst.at[rows(me * t, t)], sem, tgt)
                send(src.at[:, col(S + lax.div(tgt, G))], dst.at[rows(L + me * t, t)], sem, tgt)
            return carry

        lax.fori_loop(1, S, to_peer, 0)

    send_pair(((kc_hbm, kc_all, 0), (vc_hbm, vc_all, 1)))

    def project(which, out_fn, first_tile, next_w):
        def body(i, carry):
            step = which * tiles + i
            slot = lax.rem(step, NBUF)
            fetch(weights[which], i, slot).wait()
            acc = jnp.dot(out_fn[0][...], wbuf[slot], preferred_element_type=jnp.float32).astype(jnp.bfloat16)
            ahead = i + NBUF - 1
            nslot = lax.rem(step + NBUF - 1, NBUF)

            @pl.when(ahead < tiles)
            def _():
                fetch(weights[which], ahead, nslot).start()

            if next_w is not None:
                @pl.when(ahead >= tiles)
                def _():
                    fetch(next_w, ahead - tiles, nslot).start()

            out_fn[1](i, acc)
            return carry

        lax.fori_loop(first_tile, tiles, body, 0)

    def store_rope(dst):
        def put(i, val):
            for h in range(COLS // head_dim):
                piece = val[:, h * head_dim:(h + 1) * head_dim].astype(jnp.float32)
                turned = piece * cos_ref[...] + pltpu.roll(piece, head_dim // 2, 1) * sin_ref[...]
                dst[:, pl.ds(pl.multiple_of(i * COLS + h * head_dim, head_dim), head_dim)] = turned.astype(jnp.bfloat16)
        return put

    def store_plain(dst):
        def put(i, val):
            dst[:, pl.ds(pl.multiple_of(i * COLS, COLS), COLS)] = val
        return put

    project(0, (x_ref, store_rope(q_loc)), 0, wk_hbm)

    local(q_loc.at[:, col(me)], q_all.at[rows(me * t, t)], 2)

    def q_peer(d, carry):
        tgt = lax.rem(me + d, S)
        send(q_loc.at[:, col(tgt)], q_all.at[rows(me * t, t)], 2, tgt)
        return carry

    lax.fori_loop(1, S, q_peer, 0)
    xrow = L + jnp.where(hi_share, per * t, 0) + lax.rem(me, per) * t

    def q_extra(g, carry):
        tgt = g * G + my_rank

        @pl.when(tgt == me)
        def _():
            local(q_loc.at[:, col(S + g)], q_all.at[rows(xrow, t)], 2)

        @pl.when(tgt != me)
        def _():
            send(q_loc.at[:, col(S + g)], q_all.at[rows(xrow, t)], 2, tgt)
        return carry

    lax.fori_loop(0, E, q_extra, 0)

    project(1, (x_ref, store_rope(kn_ref)), 0, wv_hbm)
    send_pair(((kn_ref, kn_all, 3),))
    project(2, (x_ref, store_plain(vn_ref)), 0, wo_hbm)
    send_pair(((vn_ref, vn_all, 4),))

    nmain = L // QB
    nq = nmain + 2 * per * t // QB

    def block_pos(qb):
        return jnp.where(qb < nmain, qb, jnp.where(qb == nmain, rank, 2 * G - 1 - rank))

    wait_recv(q_all, 2)
    wait_recv(kc_all, 0)
    wait_recv(vc_all, 1)

    def cache_block(qb, carry):
        base = jnp.where(qb < nmain, 0, L)
        qs = [q_all[rows(qb * QB + c * QC, QC), :] for c in range(2)]

        def step(j, state):
            k = kc_all[rows(base + j * KB, KB), :]
            v = vc_all[rows(base + j * KB, KB), :]
            return tuple(online_step(qs[c], k, v, *state[c], coef) for c in range(2))

        init = tuple((jnp.full((QC, 1), -jnp.inf, jnp.float32), jnp.zeros((QC, 128), jnp.float32),
                      jnp.zeros((QC, head_dim), jnp.float32)) for _ in range(2))
        state = lax.fori_loop(0, L // KB, step, init)
        for c in range(2):
            r = rows(qb * QB + c * QC, QC)
            m_st[r, :], l_st[r, :], acc_st[r, :] = state[c]
        return carry

    lax.fori_loop(0, nq, cache_block, 0)

    wait_recv(kn_all, 3)
    wait_recv(vn_all, 4)

    def send_out(qb):
        head = jnp.where(qb < nmain, me, xhead)
        for piece in range(QB // t):
            tgt = block_pos(qb) * (QB // t) + piece
            src = o_all.at[rows(qb * QB + piece * t, t)]
            dst = o_loc.at[:, col(head)]

            @pl.when(tgt == me)
            def _():
                local(src, dst, 5)

            @pl.when(tgt != me)
            def _():
                send(src, dst, 5, tgt)

    def new_block(qb, carry):
        base = jnp.where(qb < nmain, 0, L)
        pos = block_pos(qb)
        r = [rows(qb * QB + c * QC, QC) for c in range(2)]
        qs = [q_all[r[c], :] for c in range(2)]
        init = tuple((m_st[r[c], :], l_st[r[c], :], acc_st[r[c], :]) for c in range(2))

        def step(j, state):
            k = kn_all[rows(base + j * QB, QB), :]
            v = vn_all[rows(base + j * QB, QB), :]
            return tuple(online_step(qs[c], k, v, *state[c], coef) for c in range(2))

        state = lax.fori_loop(0, pos, step, init)
        for c in range(2):
            span = (c + 1) * QC
            k = kn_all[rows(base + pos * QB, span), :]
            v = vn_all[rows(base + pos * QB, span), :]
            mask = (lax.broadcasted_iota(jnp.int32, (QC, span), 1)
                    <= lax.broadcasted_iota(jnp.int32, (QC, span), 0) + c * QC)
            _, l, acc = online_step(qs[c], k, v, *state[c], coef, mask)
            o_all[r[c], :] = (acc / jnp.sum(l, axis=1, keepdims=True)).astype(jnp.bfloat16)

        @pl.when(qb > 0)
        def _():
            send_out(qb - 1)
        return carry

    lax.fori_loop(0, nq, new_block, 0)
    send_out(nq - 1)

    wait_recv(o_loc, 5)
    project(3, (o_loc, store_plain(y_ref)), 0, None)

    for buf, sem in ((kc_all, 0), (vc_all, 1), (kn_all, 3), (vn_all, 4)):
        wait_sent(buf, 2 * (S - 1), sem)
    for sem in (2, 5):
        wait_sent(q_all, S - 1, sem)

        @pl.when(own_extra)
        def _():
            wait_sent(q_all, E - 1, sem)

        @pl.when(jnp.logical_not(own_extra))
        def _():
            wait_sent(q_all, E, sem)


def solution(mesh):
    sp, cp = mesh.shape['sp'], mesh.shape['cp']
    S = sp * cp
    row_spec = P(('dp', 'sp', 'cp'))

    def local_fn(x_loc, kc_loc, vc_loc, w_q, w_k, w_v, w_o):
        t, d_model = x_loc.shape
        _, heads, hd = kc_loc.shape
        G = S // (heads - S)
        L, X = S * t, S * t // G
        width = heads * hd
        seq_idx = lax.axis_index('sp') * cp + lax.axis_index('cp')
        cos_t, sin_t = rope_tables(L + seq_idx * t + jnp.arange(t), hd)
        bf, f32 = jnp.bfloat16, jnp.float32
        vmem, hbm = pl.BlockSpec(memory_space=pltpu.VMEM), pl.BlockSpec(memory_space=pl.ANY)
        y, k_new, v_new = pl.pallas_call(
            functools.partial(kernel, sp, cp, heads, hd),
            out_shape=[jax.ShapeDtypeStruct((t, d_model), bf), jax.ShapeDtypeStruct((t, width), bf),
                       jax.ShapeDtypeStruct((t, width), bf)],
            in_specs=[vmem, vmem, vmem] + [hbm] * 6,
            out_specs=[vmem] * 3,
            scratch_shapes=[
                pltpu.VMEM((t, width), bf),
                pltpu.VMEM((L + X, hd), bf),
                pltpu.VMEM((2 * L, hd), bf), pltpu.VMEM((2 * L, hd), bf),
                pltpu.VMEM((2 * L, hd), bf), pltpu.VMEM((2 * L, hd), bf),
                pltpu.VMEM((L + X, hd), bf),
                pltpu.VMEM((t, width), bf),
                pltpu.VMEM((L + X, 1), f32), pltpu.VMEM((L + X, 128), f32), pltpu.VMEM((L + X, hd), f32),
                pltpu.VMEM((NBUF, d_model, COLS), bf),
                pltpu.SemaphoreType.DMA((NBUF,)),
                pltpu.SemaphoreType.DMA((6,)),
                pltpu.SemaphoreType.DMA((6,)),
            ],
            compiler_params=pltpu.CompilerParams(collective_id=0, has_side_effects=True, vmem_limit_bytes=67043328),
        )(x_loc, cos_t, sin_t, kc_loc.reshape(t, width), vc_loc.reshape(t, width), w_q, w_k, w_v, w_o)
        return y, k_new.reshape(t, heads, hd), v_new.reshape(t, heads, hd)

    return jax.shard_map(local_fn, mesh=mesh, in_specs=(row_spec, row_spec, row_spec, P(), P(), P(), P()), out_specs=(row_spec, row_spec, row_spec), check_vma=False)
```

```python
import functools
import math

import jax
import jax.numpy as jnp
from jax import lax
from jax.experimental import pallas as pl
from jax.experimental.pallas import tpu as pltpu
from jax.sharding import PartitionSpec as P

ROPE_BASE = 500000
MESH = pl.DeviceIdType.MESH
COLS = 512
NBUF = 4
QB = 512
SUB = 512
KB = 1024


def rope_tables(positions, head_dim):
    inv_freq = 1.0 / (ROPE_BASE ** (jnp.arange(0, head_dim, 2, dtype=jnp.float32) / head_dim))
    angles = positions.astype(jnp.float32)[:, None] * inv_freq[None, :]
    cos_t, sin_t = jnp.cos(angles), jnp.sin(angles)
    return jnp.concatenate([cos_t, cos_t], axis=-1), jnp.concatenate([-sin_t, sin_t], axis=-1)


def score_piece(i, q, k_at, s_buf, top, mask):
    s = lax.dot_general(k_at(i), q, (((1,), (1,)), ((), ())), preferred_element_type=jnp.float32)
    if mask is not None:
        s = jnp.where(mask(i), s, -jnp.inf)
    s_buf[i * SUB:(i + 1) * SUB, :] = s
    return jnp.maximum(top, jnp.max(s, axis=0, keepdims=True))


def online_step(s_buf, top, v_at, state, coef, pieces, ahead):
    m, l, acc = state
    m_new = jnp.maximum(m, top)
    alpha = jnp.exp2((m - m_new) * coef)
    l, acc = l * alpha, acc * alpha
    top_next = jnp.full_like(m, -jnp.inf)
    for i in range(pieces):
        top_next = score_piece(i, *ahead[:3], top_next, ahead[3])
        p = jnp.exp2((s_buf[i * SUB:(i + 1) * SUB, :] - m_new) * coef)
        l = l + jnp.sum(p.reshape(-1, 8, p.shape[1]), axis=0)
        acc = acc + jnp.dot(v_at(i), p.astype(jnp.bfloat16), preferred_element_type=jnp.float32)
    return (m_new, l, acc), top_next


def kernel(sp, cp, heads, head_dim,
           x_ref, cos_ref, sin_ref, kc_hbm, vc_hbm, wq_hbm, wk_hbm, wv_hbm, wo_hbm,
           y_ref, kn_ref, vn_ref,
           q_loc, vt_loc, q_all, kc_all, vc_all, kn_all, vn_all, o_all, o_loc,
           m_st, l_st, acc_st, s_a, s_b, s_c, wbuf, wsem, ssem, rsem):
    S = sp * cp
    E = heads - S
    G = S // E
    t = x_ref.shape[0]
    d_model = x_ref.shape[1]
    L = S * t
    me = lax.axis_index('sp') * cp + lax.axis_index('cp')
    per = S // (2 * G)
    rank = lax.rem(me, G)
    xhead = S + lax.div(me, G)
    my_blk = lax.div(me, per)
    my_rank = jnp.minimum(my_blk, 2 * G - 1 - my_blk)
    hi_share = my_blk >= G
    own_extra = my_rank == rank
    coef = (head_dim ** -0.5) * math.log2(math.e)

    X = cp // 2
    my_y, my_x, my_core = lax.div(me, cp), lax.div(lax.rem(me, cp), 2), lax.rem(me, 2)

    def peer(d):
        core, chip = lax.div(d, S // 2), lax.rem(d, S // 2)
        dx = lax.rem(chip, X)
        dy = lax.rem(lax.div(chip, X) + dx, sp)
        return lax.rem(my_y + dy, sp) * cp + lax.rem(my_x + dx, X) * 2 + lax.rem(my_core + core, 2)

    def dev(idx):
        return {'sp': lax.div(idx, cp), 'cp': lax.rem(idx, cp)}

    def col(h):
        return pl.ds(pl.multiple_of(h * head_dim, head_dim), head_dim)

    def rows(start, size):
        return pl.ds(pl.multiple_of(start, 128), size)

    def send(src, dst, sem, tgt):
        pltpu.make_async_remote_copy(src_ref=src, dst_ref=dst, send_sem=ssem.at[sem], recv_sem=rsem.at[sem],
                                     device_id=dev(tgt), device_id_type=MESH).start()

    def local(src, dst, sem):
        pltpu.make_async_copy(src, dst, rsem.at[sem]).start()

    def wait_recv(buf, sem):
        pltpu.make_async_copy(buf, buf, rsem.at[sem]).wait()

    def wait_sent(buf, n_pieces, sem):
        part = buf.at[pl.ds(0, n_pieces * t)]
        pltpu.make_async_copy(part, part, ssem.at[sem]).wait()

    tiles = d_model // COLS
    weights = (wq_hbm, wk_hbm, wv_hbm, wo_hbm)

    def fetch(w, tile, slot):
        return pltpu.make_async_copy(w.at[:, pl.ds(pl.multiple_of(tile * COLS, COLS), COLS)], wbuf.at[slot], wsem.at[slot])

    for tile in range(NBUF - 1):
        fetch(wq_hbm, tile, tile).start()

    barrier = pltpu.get_barrier_semaphore()

    def greet(d, carry):
        pl.semaphore_signal(barrier, inc=1, device_id=dev(lax.rem(me + d, S)), device_id_type=MESH)
        return carry

    lax.fori_loop(1, S, greet, 0)
    pl.semaphore_wait(barrier, S - 1)

    def head_of(sel, idx):
        return idx if sel == 0 else S + lax.div(idx, G)

    def k_piece(src, dst, sel, idx):
        return src.at[:, col(head_of(sel, idx))], dst.at[rows(sel * L + me * t, t)]

    def v_piece(src, dst, sel, idx):
        return (src.at[rows(head_of(sel, idx) * head_dim, head_dim)],
                dst.at[pl.ds(sel * head_dim, head_dim), rows(me * t, t)])

    def send_all(groups):
        for piece, src, dst, sem in groups:
            for sel in range(2):
                local(*piece(src, dst, sel, me), sem)
        for piece, src, dst, sem in groups:
            for sel in range(2):
                def to_peer(d, carry, piece=piece, src=src, dst=dst, sem=sem, sel=sel):
                    tgt = peer(d)
                    send(*piece(src, dst, sel, tgt), sem, tgt)
                    return carry

                lax.fori_loop(1, S, to_peer, 0)

    send_all(((k_piece, kc_hbm, kc_all, 0), (v_piece, vc_hbm, vc_all, 1)))

    def project(which, out_fn, first_tile, next_w):
        def body(i, carry):
            step = which * tiles + i
            slot = lax.rem(step, NBUF)
            fetch(weights[which], i, slot).wait()
            acc = jnp.dot(out_fn[0][...], wbuf[slot], preferred_element_type=jnp.float32).astype(jnp.bfloat16)
            ahead = i + NBUF - 1
            nslot = lax.rem(step + NBUF - 1, NBUF)

            @pl.when(ahead < tiles)
            def _():
                fetch(weights[which], ahead, nslot).start()

            if next_w is not None:
                @pl.when(ahead >= tiles)
                def _():
                    fetch(next_w, ahead - tiles, nslot).start()

            out_fn[1](i, acc)
            return carry

        lax.fori_loop(first_tile, tiles, body, 0)

    def store_rope(dst):
        def put(i, val):
            for h in range(COLS // head_dim):
                piece = val[:, h * head_dim:(h + 1) * head_dim].astype(jnp.float32)
                turned = piece * cos_ref[...] + pltpu.roll(piece, head_dim // 2, 1) * sin_ref[...]
                dst[:, pl.ds(pl.multiple_of(i * COLS + h * head_dim, head_dim), head_dim)] = turned.astype(jnp.bfloat16)
        return put

    def store_plain(dst):
        def put(i, val):
            dst[:, pl.ds(pl.multiple_of(i * COLS, COLS), COLS)] = val
        return put

    def store_values(i, val):
        vn_ref[:, pl.ds(pl.multiple_of(i * COLS, COLS), COLS)] = val
        vt_loc[pl.ds(pl.multiple_of(i * COLS, COLS), COLS), :] = val.T

    project(0, (x_ref, store_rope(q_loc)), 0, wk_hbm)

    local(q_loc.at[:, col(me)], q_all.at[rows(me * t, t)], 2)

    def q_peer(d, carry):
        tgt = peer(d)
        send(q_loc.at[:, col(tgt)], q_all.at[rows(me * t, t)], 2, tgt)
        return carry

    lax.fori_loop(1, S, q_peer, 0)
    xrow = L + jnp.where(hi_share, per * t, 0) + lax.rem(me, per) * t

    def q_extra(g, carry):
        tgt = g * G + my_rank

        @pl.when(tgt == me)
        def _():
            local(q_loc.at[:, col(S + g)], q_all.at[rows(xrow, t)], 2)

        @pl.when(tgt != me)
        def _():
            send(q_loc.at[:, col(S + g)], q_all.at[rows(xrow, t)], 2, tgt)
        return carry

    lax.fori_loop(0, E, q_extra, 0)

    project(1, (x_ref, store_rope(kn_ref)), 0, wv_hbm)
    send_all(((k_piece, kn_ref, kn_all, 3),))
    project(2, (x_ref, store_values), 0, wo_hbm)
    send_all(((v_piece, vt_loc, vn_all, 4),))

    nmain = L // QB
    nq = nmain + 2 * per * t // QB

    def block_pos(qb):
        return jnp.where(qb < nmain, qb, jnp.where(qb == nmain, rank, 2 * G - 1 - rank))

    wait_recv(q_all, 2)
    wait_recv(kc_all, 0)
    wait_recv(vc_all, 1)

    bufs = (s_a, s_b, s_c)

    def k_rows(buf, sel, start):
        return lambda i: buf[rows(sel * L + start + i * SUB, SUB), :]

    def v_cols(buf, sel, start):
        return lambda i: buf[rows(sel * head_dim, head_dim), rows(start + i * SUB, SUB)]

    def first_scores(q, k_at, s_buf, pieces):
        top = jnp.full((1, QB), -jnp.inf, jnp.float32)
        for i in range(pieces):
            top = score_piece(i, q, k_at, s_buf, top, None)
        return top

    def query(qb):
        return q_all[rows(qb * QB, QB), :]

    nst = L // KB

    def cache_block(qb, top):
        sel, after = lax.div(qb, nmain), jnp.minimum(qb + 1, nq - 1)
        q, q_after = query(qb), query(after)
        state = (jnp.full((1, QB), -jnp.inf, jnp.float32), jnp.zeros((8, QB), jnp.float32),
                 jnp.zeros((head_dim, QB), jnp.float32))
        for j in range(nst):
            if j + 1 < nst:
                ahead = (q, k_rows(kc_all, sel, (j + 1) * KB), bufs[(j + 1) % 2], None)
            else:
                ahead = (q_after, k_rows(kc_all, lax.div(after, nmain), 0), bufs[0], None)
            state, top = online_step(bufs[j % 2], top, v_cols(vc_all, sel, j * KB), state, coef, KB // SUB, ahead)
        m_st[qb, 0:1, :], l_st[qb], acc_st[qb] = state
        return top

    lax.fori_loop(0, nq, cache_block, first_scores(query(0), k_rows(kc_all, 0, 0), s_a, KB // SUB))

    wait_recv(kn_all, 3)
    wait_recv(vn_all, 4)

    def send_out(qb):
        head = jnp.where(qb < nmain, me, xhead)
        for piece in range(QB // t):
            tgt = block_pos(qb) * (QB // t) + piece
            src = o_all.at[rows(qb * QB + piece * t, t)]
            dst = o_loc.at[:, col(head)]

            @pl.when(tgt == me)
            def _():
                local(src, dst, 5)

            @pl.when(tgt != me)
            def _():
                send(src, dst, 5, tgt)

    nfull = nmain - 1

    def item(i, n):
        qa = jnp.where(i < nmain // 2, i, nmain)
        qb = jnp.where(i < nmain // 2, nmain - 1 - i, nmain + 1)
        pa, pb = block_pos(qa), block_pos(qb)
        if n < nfull:
            early = n < pa
            return jnp.where(early, qa, qb), jnp.where(early, n, n - pa), None
        blk, pos = (qa, pa) if n == nfull else (qb, pb)
        return blk, pos, lambda piece: (lax.broadcasted_iota(jnp.int32, (SUB, QB), 0) + piece * SUB
                                        <= lax.broadcasted_iota(jnp.int32, (SUB, QB), 1))

    def new_pair(i, top):
        after = jnp.minimum(i + 1, nq // 2 - 1)
        for n in range(nfull + 2):
            blk, pos, _ = item(i, n)
            nblk, npos, nmask = item(i, n + 1) if n + 1 < nfull + 2 else item(after, 0)
            ahead = (query(nblk), k_rows(kn_all, lax.div(nblk, nmain), npos * QB), bufs[(n + 1) % 3], nmask)
            state = (m_st[blk, 0:1, :], l_st[blk], acc_st[blk])
            state, top = online_step(bufs[n % 3], top, v_cols(vn_all, lax.div(blk, nmain), pos * QB), state, coef,
                                     QB // SUB, ahead)
            if n < nfull:
                m_st[blk, 0:1, :], l_st[blk], acc_st[blk] = state
            else:
                out = (state[2] / jnp.sum(state[1], axis=0, keepdims=True)).astype(jnp.bfloat16)
                o_all[rows(blk * QB, QB), :] = out.T

        @pl.when(i > 0)
        def _():
            send_out(item(i - 1, nfull)[0])
            send_out(item(i - 1, nfull + 1)[0])
        return top

    blk0, pos0, _ = item(0, 0)
    lax.fori_loop(0, nq // 2, new_pair,
                  first_scores(query(blk0), k_rows(kn_all, lax.div(blk0, nmain), pos0 * QB), s_a, QB // SUB))
    send_out(item(nq // 2 - 1, nfull)[0])
    send_out(item(nq // 2 - 1, nfull + 1)[0])

    wait_recv(o_loc, 5)
    project(3, (o_loc, store_plain(y_ref)), 0, None)

    for sem in (0, 1, 3, 4):
        wait_sent(kc_all, 2 * (S - 1), sem)
    for sem in (2, 5):
        wait_sent(q_all, S - 1, sem)

        @pl.when(own_extra)
        def _():
            wait_sent(q_all, E - 1, sem)

        @pl.when(jnp.logical_not(own_extra))
        def _():
            wait_sent(q_all, E, sem)


def solution(mesh):
    sp, cp = mesh.shape['sp'], mesh.shape['cp']
    S = sp * cp
    row_spec = P(('dp', 'sp', 'cp'))

    def local_fn(x_loc, kc_loc, vc_loc, w_q, w_k, w_v, w_o):
        t, d_model = x_loc.shape
        _, heads, hd = kc_loc.shape
        G = S // (heads - S)
        L, X = S * t, S * t // G
        width = heads * hd
        chains = (L + X) // QB
        seq_idx = lax.axis_index('sp') * cp + lax.axis_index('cp')
        cos_t, sin_t = rope_tables(L + seq_idx * t + jnp.arange(t), hd)
        bf, f32 = jnp.bfloat16, jnp.float32
        vmem, hbm = pl.BlockSpec(memory_space=pltpu.VMEM), pl.BlockSpec(memory_space=pl.ANY)
        y, k_new, v_new = pl.pallas_call(
            functools.partial(kernel, sp, cp, heads, hd),
            out_shape=[jax.ShapeDtypeStruct((t, d_model), bf), jax.ShapeDtypeStruct((t, width), bf),
                       jax.ShapeDtypeStruct((t, width), bf)],
            in_specs=[vmem, vmem, vmem] + [hbm] * 6,
            out_specs=[vmem] * 3,
            scratch_shapes=[
                pltpu.VMEM((t, width), bf), pltpu.VMEM((width, t), bf),
                pltpu.VMEM((L + X, hd), bf),
                pltpu.VMEM((2 * L, hd), bf), pltpu.VMEM((2 * hd, L), bf),
                pltpu.VMEM((2 * L, hd), bf), pltpu.VMEM((2 * hd, L), bf),
                pltpu.VMEM((L + X, hd), bf),
                pltpu.VMEM((t, width), bf),
                pltpu.VMEM((chains, 8, QB), f32), pltpu.VMEM((chains, 8, QB), f32), pltpu.VMEM((chains, hd, QB), f32),
                pltpu.VMEM((KB, QB), f32), pltpu.VMEM((KB, QB), f32), pltpu.VMEM((QB, QB), f32),
                pltpu.VMEM((NBUF, d_model, COLS), bf),
                pltpu.SemaphoreType.DMA((NBUF,)),
                pltpu.SemaphoreType.DMA((6,)),
                pltpu.SemaphoreType.DMA((6,)),
            ],
            compiler_params=pltpu.CompilerParams(collective_id=0, has_side_effects=True, vmem_limit_bytes=67043328),
        )(x_loc, cos_t, sin_t, kc_loc.reshape(t, width), vc_loc.transpose(1, 2, 0).reshape(width, t), w_q, w_k, w_v, w_o)
        return y, k_new.reshape(t, heads, hd), v_new.reshape(t, heads, hd)

    return jax.shard_map(local_fn, mesh=mesh, in_specs=(row_spec, row_spec, row_spec, P(), P(), P(), P()), out_specs=(row_spec, row_spec, row_spec), check_vma=False)
```

```python
import functools
import math

import jax
import jax.numpy as jnp
from jax import lax
from jax.experimental import pallas as pl
from jax.experimental.pallas import tpu as pltpu
from jax.sharding import PartitionSpec as P

ROPE_BASE = 500000
MESH = pl.DeviceIdType.MESH
COLS = 512
NBUF = 6
QB = 512
SUB = 512
KB = 1024


def rope_tables(positions, head_dim):
    inv_freq = 1.0 / (ROPE_BASE ** (jnp.arange(0, head_dim, 2, dtype=jnp.float32) / head_dim))
    angles = positions.astype(jnp.float32)[:, None] * inv_freq[None, :]
    cos_t, sin_t = jnp.cos(angles), jnp.sin(angles)
    return jnp.concatenate([cos_t, cos_t], axis=-1), jnp.concatenate([-sin_t, sin_t], axis=-1)


def score_piece(i, q, k_at, s_buf, top, mask):
    s = lax.dot_general(k_at(i), q, (((1,), (1,)), ((), ())), preferred_element_type=jnp.float32)
    if mask is not None:
        s = jnp.where(mask(i), s, -jnp.inf)
    s_buf[i * SUB:(i + 1) * SUB, :] = s
    return jnp.maximum(top, jnp.max(s, axis=0, keepdims=True))


def online_step(s_buf, top, v_at, state, coef, pieces, ahead):
    m, l, acc = state
    m_new = jnp.maximum(m, top)
    alpha = jnp.exp2((m - m_new) * coef)
    l, acc = l * alpha, acc * alpha
    top_next = jnp.full_like(m, -jnp.inf)
    for i in range(pieces):
        top_next = score_piece(i, *ahead[:3], top_next, ahead[3])
        p = jnp.exp2((s_buf[i * SUB:(i + 1) * SUB, :] - m_new) * coef)
        l = l + jnp.sum(p.reshape(-1, 8, p.shape[1]), axis=0)
        acc = acc + jnp.dot(v_at(i), p.astype(jnp.bfloat16), preferred_element_type=jnp.float32)
    return (m_new, l, acc), top_next


def kernel(sp, cp, heads, head_dim,
           x_ref, cos_ref, sin_ref, kc_hbm, vc_hbm, wq_hbm, wk_hbm, wv_hbm, wo_hbm,
           y_ref, kn_ref, vn_ref,
           q_loc, vt_loc, q_all, kc_all, vc_all, kn_all, vn_all, o_all, o_loc,
           m_st, l_st, acc_st, s_a, s_b, s_c, wbuf, wsem, ssem, rsem):
    S = sp * cp
    E = heads - S
    G = S // E
    t = x_ref.shape[0]
    d_model = x_ref.shape[1]
    L = S * t
    me = lax.axis_index('sp') * cp + lax.axis_index('cp')
    per = S // (2 * G)
    rank = lax.rem(me, G)
    xhead = S + lax.div(me, G)
    my_blk = lax.div(me, per)
    my_rank = jnp.minimum(my_blk, 2 * G - 1 - my_blk)
    hi_share = my_blk >= G
    own_extra = my_rank == rank
    coef = (head_dim ** -0.5) * math.log2(math.e)

    X = cp // 2
    my_y, my_x, my_core = lax.div(me, cp), lax.div(lax.rem(me, cp), 2), lax.rem(me, 2)

    def peer(d):
        core, chip = lax.div(d, S // 2), lax.rem(d, S // 2)
        dx = lax.rem(chip, X)
        dy = lax.rem(lax.div(chip, X) + dx, sp)
        return lax.rem(my_y + dy, sp) * cp + lax.rem(my_x + dx, X) * 2 + lax.rem(my_core + core, 2)

    def dev(idx):
        return {'sp': lax.div(idx, cp), 'cp': lax.rem(idx, cp)}

    def col(h):
        return pl.ds(pl.multiple_of(h * head_dim, head_dim), head_dim)

    def rows(start, size):
        return pl.ds(pl.multiple_of(start, 128), size)

    def send(src, dst, sem, tgt):
        pltpu.make_async_remote_copy(src_ref=src, dst_ref=dst, send_sem=ssem.at[sem], recv_sem=rsem.at[sem],
                                     device_id=dev(tgt), device_id_type=MESH).start()

    def local(src, dst, sem):
        pltpu.make_async_copy(src, dst, rsem.at[sem]).start()

    def wait_recv(buf, sem):
        pltpu.make_async_copy(buf, buf, rsem.at[sem]).wait()

    def wait_sent(buf, n_pieces, sem):
        part = buf.at[pl.ds(0, n_pieces * t)]
        pltpu.make_async_copy(part, part, ssem.at[sem]).wait()

    tiles = d_model // COLS
    weights = (wq_hbm, wk_hbm, wv_hbm, wo_hbm)

    def fetch(w, tile, slot):
        return pltpu.make_async_copy(w.at[:, pl.ds(pl.multiple_of(tile * COLS, COLS), COLS)], wbuf.at[slot], wsem.at[slot])

    for tile in range(NBUF - 1):
        fetch(wq_hbm, tile, tile).start()

    barrier = pltpu.get_barrier_semaphore()

    def greet(d, carry):
        pl.semaphore_signal(barrier, inc=1, device_id=dev(lax.rem(me + d, S)), device_id_type=MESH)
        return carry

    lax.fori_loop(1, S, greet, 0)
    pl.semaphore_wait(barrier, S - 1)

    def head_of(sel, idx):
        return idx if sel == 0 else S + lax.div(idx, G)

    def k_piece(src, dst, sel, idx):
        return src.at[:, col(head_of(sel, idx))], dst.at[rows(sel * L + me * t, t)]

    def v_piece(src, dst, sel, idx):
        return (src.at[rows(head_of(sel, idx) * head_dim, head_dim)],
                dst.at[pl.ds(sel * head_dim, head_dim), rows(me * t, t)])

    def send_all(piece, src, dst, sem, sel):
        local(*piece(src, dst, sel, me), sem)

        def to_peer(d, carry):
            tgt = peer(d)
            send(*piece(src, dst, sel, tgt), sem, tgt)
            return carry

        lax.fori_loop(1, S if sel == 0 else S // 2, to_peer, 0)

    def pass_on(piece, dst, sem):
        def body(n, carry):
            region = piece(dst, dst, 1, 2 * n + my_core)
            send(region, region, sem, me + 1 - 2 * my_core)
            return carry

        lax.fori_loop(0, S // 2, body, 0)

    def k_region(_, dst, sel, idx):
        return dst.at[rows(sel * L + idx * t, t)]

    def v_region(_, dst, sel, idx):
        return dst.at[pl.ds(sel * head_dim, head_dim), rows(idx * t, t)]

    send_all(k_piece, kc_hbm, kc_all, 0, 0)
    send_all(v_piece, vc_hbm, vc_all, 1, 0)
    send_all(k_piece, kc_hbm, kc_all, 6, 1)
    send_all(v_piece, vc_hbm, vc_all, 7, 1)

    def project(which, out_fn, first_tile, next_w):
        def body(i, carry):
            step = which * tiles + i
            slot = lax.rem(step, NBUF)
            fetch(weights[which], i, slot).wait()
            acc = jnp.dot(out_fn[0][...], wbuf[slot], preferred_element_type=jnp.float32).astype(jnp.bfloat16)
            ahead = i + NBUF - 1
            nslot = lax.rem(step + NBUF - 1, NBUF)

            @pl.when(ahead < tiles)
            def _():
                fetch(weights[which], ahead, nslot).start()

            if next_w is not None:
                @pl.when(ahead >= tiles)
                def _():
                    fetch(next_w, ahead - tiles, nslot).start()

            out_fn[1](i, acc)
            return carry

        lax.fori_loop(first_tile, tiles, body, 0)

    def store_rope(dst):
        def put(i, val):
            for h in range(COLS // head_dim):
                piece = val[:, h * head_dim:(h + 1) * head_dim].astype(jnp.float32)
                turned = piece * cos_ref[...] + pltpu.roll(piece, head_dim // 2, 1) * sin_ref[...]
                dst[:, pl.ds(pl.multiple_of(i * COLS + h * head_dim, head_dim), head_dim)] = turned.astype(jnp.bfloat16)
        return put

    def store_plain(dst):
        def put(i, val):
            dst[:, pl.ds(pl.multiple_of(i * COLS, COLS), COLS)] = val
        return put

    def store_values(i, val):
        vn_ref[:, pl.ds(pl.multiple_of(i * COLS, COLS), COLS)] = val
        vt_loc[pl.ds(pl.multiple_of(i * COLS, COLS), COLS), :] = val.T

    project(0, (x_ref, store_rope(q_loc)), 0, wk_hbm)

    local(q_loc.at[:, col(me)], q_all.at[rows(me * t, t)], 2)

    def q_peer(d, carry):
        tgt = peer(d)
        send(q_loc.at[:, col(tgt)], q_all.at[rows(me * t, t)], 2, tgt)
        return carry

    lax.fori_loop(1, S, q_peer, 0)
    xrow = L + jnp.where(hi_share, per * t, 0) + lax.rem(me, per) * t

    def q_extra(g, carry):
        tgt = g * G + my_rank

        @pl.when(tgt == me)
        def _():
            local(q_loc.at[:, col(S + g)], q_all.at[rows(xrow, t)], 2)

        @pl.when(tgt != me)
        def _():
            send(q_loc.at[:, col(S + g)], q_all.at[rows(xrow, t)], 2, tgt)
        return carry

    lax.fori_loop(0, E, q_extra, 0)

    project(1, (x_ref, store_rope(kn_ref)), 0, wv_hbm)
    send_all(k_piece, kn_ref, kn_all, 3, 0)
    project(2, (x_ref, store_values), 0, wo_hbm)
    send_all(v_piece, vt_loc, vn_all, 4, 0)
    send_all(k_piece, kn_ref, kn_all, 8, 1)
    send_all(v_piece, vt_loc, vn_all, 9, 1)

    nmain = L // QB
    nq = nmain + 2 * per * t // QB

    def block_pos(qb):
        return jnp.where(qb < nmain, qb, jnp.where(qb == nmain, rank, 2 * G - 1 - rank))

    wait_recv(q_all, 2)
    main_part, half_part = kc_all.at[pl.ds(0, L)], kc_all.at[pl.ds(0, L // 2)]
    wait_recv(main_part, 0)
    wait_recv(main_part, 1)
    wait_recv(half_part, 6)
    wait_recv(half_part, 7)
    pass_on(k_region, kc_all, 10)
    pass_on(v_region, vc_all, 11)

    bufs = (s_a, s_b, s_c)

    def k_rows(buf, sel, start):
        return lambda i: buf[rows(sel * L + start + i * SUB, SUB), :]

    def v_cols(buf, sel, start):
        return lambda i: buf[rows(sel * head_dim, head_dim), rows(start + i * SUB, SUB)]

    def first_scores(q, k_at, s_buf, pieces):
        top = jnp.full((1, QB), -jnp.inf, jnp.float32)
        for i in range(pieces):
            top = score_piece(i, q, k_at, s_buf, top, None)
        return top

    def query(qb):
        return q_all[rows(qb * QB, QB), :]

    nst = L // KB

    def cache_block(sel, last, qb, top):
        after = jnp.minimum(qb + 1, last)
        q, q_after = query(qb), query(after)
        state = (jnp.full((1, QB), -jnp.inf, jnp.float32), jnp.zeros((8, QB), jnp.float32),
                 jnp.zeros((head_dim, QB), jnp.float32))
        for j in range(nst):
            if j + 1 < nst:
                ahead = (q, k_rows(kc_all, sel, (j + 1) * KB), bufs[(j + 1) % 2], None)
            else:
                ahead = (q_after, k_rows(kc_all, sel, 0), bufs[0], None)
            state, top = online_step(bufs[j % 2], top, v_cols(vc_all, sel, j * KB), state, coef, KB // SUB, ahead)
        m_st[qb, 0:1, :], l_st[qb], acc_st[qb] = state
        return top

    def cache_part(sel, carry):
        @pl.when(sel == 1)
        def _():
            wait_recv(half_part, 10)
            wait_recv(half_part, 11)

        start, stop = sel * nmain, jnp.where(sel == 0, nmain, nq)
        lax.fori_loop(start, stop, functools.partial(cache_block, sel, stop - 1),
                      first_scores(query(start), k_rows(kc_all, sel, 0), s_a, KB // SUB))
        return carry

    lax.fori_loop(0, 2, cache_part, 0)

    wait_recv(main_part, 3)
    wait_recv(main_part, 4)

    def send_out(qb):
        head = jnp.where(qb < nmain, me, xhead)
        for piece in range(QB // t):
            tgt = block_pos(qb) * (QB // t) + piece
            src = o_all.at[rows(qb * QB + piece * t, t)]
            dst = o_loc.at[:, col(head)]

            @pl.when(tgt == me)
            def _():
                local(src, dst, 5)

            @pl.when(tgt != me)
            def _():
                send(src, dst, 5, tgt)

    nfull = nmain - 1

    def item(i, n):
        qa = jnp.where(i < nmain // 2, i, nmain)
        qb = jnp.where(i < nmain // 2, nmain - 1 - i, nmain + 1)
        pa, pb = block_pos(qa), block_pos(qb)
        if n < nfull:
            early = n < pa
            return jnp.where(early, qa, qb), jnp.where(early, n, n - pa), None
        blk, pos = (qa, pa) if n == nfull else (qb, pb)
        return blk, pos, lambda piece: (lax.broadcasted_iota(jnp.int32, (SUB, QB), 0) + piece * SUB
                                        <= lax.broadcasted_iota(jnp.int32, (SUB, QB), 1))

    def new_pair(sel, last, i, top):
        after = jnp.minimum(i + 1, last)
        for n in range(nfull + 2):
            blk, pos, _ = item(i, n)
            nblk, npos, nmask = item(i, n + 1) if n + 1 < nfull + 2 else item(after, 0)
            ahead = (query(nblk), k_rows(kn_all, sel, npos * QB), bufs[(n + 1) % 3], nmask)
            state = (m_st[blk, 0:1, :], l_st[blk], acc_st[blk])
            state, top = online_step(bufs[n % 3], top, v_cols(vn_all, sel, pos * QB), state, coef,
                                     QB // SUB, ahead)
            if n < nfull:
                m_st[blk, 0:1, :], l_st[blk], acc_st[blk] = state
            else:
                out = (state[2] / jnp.sum(state[1], axis=0, keepdims=True)).astype(jnp.bfloat16)
                o_all[rows(blk * QB, QB), :] = out.T

        send_out(item(i, nfull)[0])
        send_out(item(i, nfull + 1)[0])
        return top

    def new_part(sel, carry):
        @pl.when(sel == 1)
        def _():
            wait_recv(half_part, 8)
            wait_recv(half_part, 9)
            pass_on(k_region, kn_all, 12)
            pass_on(v_region, vn_all, 13)
            wait_recv(half_part, 12)
            wait_recv(half_part, 13)

        start, stop = sel * (nmain // 2), jnp.where(sel == 0, nmain // 2, nq // 2)
        blk0, pos0, _ = item(start, 0)
        lax.fori_loop(start, stop, functools.partial(new_pair, sel, stop - 1),
                      first_scores(query(blk0), k_rows(kn_all, sel, pos0 * QB), s_a, QB // SUB))
        return carry

    lax.fori_loop(0, 2, new_part, 0)

    wait_recv(o_loc, 5)
    project(3, (o_loc, store_plain(y_ref)), 0, None)

    for sem in (0, 1, 3, 4):
        wait_sent(kc_all, S - 1, sem)
    for sem in (6, 7, 8, 9):
        wait_sent(kc_all, S // 2 - 1, sem)
    for sem in (10, 11, 12, 13):
        wait_sent(kc_all, S // 2, sem)
    for sem in (2, 5):
        wait_sent(q_all, S - 1, sem)

        @pl.when(own_extra)
        def _():
            wait_sent(q_all, E - 1, sem)

        @pl.when(jnp.logical_not(own_extra))
        def _():
            wait_sent(q_all, E, sem)


def solution(mesh):
    sp, cp = mesh.shape['sp'], mesh.shape['cp']
    S = sp * cp
    row_spec = P(('dp', 'sp', 'cp'))

    def local_fn(x_loc, kc_loc, vc_loc, w_q, w_k, w_v, w_o):
        t, d_model = x_loc.shape
        _, heads, hd = kc_loc.shape
        G = S // (heads - S)
        L, X = S * t, S * t // G
        width = heads * hd
        chains = (L + X) // QB
        seq_idx = lax.axis_index('sp') * cp + lax.axis_index('cp')
        cos_t, sin_t = rope_tables(L + seq_idx * t + jnp.arange(t), hd)
        bf, f32 = jnp.bfloat16, jnp.float32
        vmem, hbm = pl.BlockSpec(memory_space=pltpu.VMEM), pl.BlockSpec(memory_space=pl.ANY)
        y, k_new, v_new = pl.pallas_call(
            functools.partial(kernel, sp, cp, heads, hd),
            out_shape=[jax.ShapeDtypeStruct((t, d_model), bf), jax.ShapeDtypeStruct((t, width), bf),
                       jax.ShapeDtypeStruct((t, width), bf)],
            in_specs=[vmem, vmem, vmem] + [hbm] * 6,
            out_specs=[vmem] * 3,
            scratch_shapes=[
                pltpu.VMEM((t, width), bf), pltpu.VMEM((width, t), bf),
                pltpu.VMEM((L + X, hd), bf),
                pltpu.VMEM((2 * L, hd), bf), pltpu.VMEM((2 * hd, L), bf),
                pltpu.VMEM((2 * L, hd), bf), pltpu.VMEM((2 * hd, L), bf),
                pltpu.VMEM((L + X, hd), bf),
                pltpu.VMEM((t, width), bf),
                pltpu.VMEM((chains, 8, QB), f32), pltpu.VMEM((chains, 8, QB), f32), pltpu.VMEM((chains, hd, QB), f32),
                pltpu.VMEM((KB, QB), f32), pltpu.VMEM((KB, QB), f32), pltpu.VMEM((QB, QB), f32),
                pltpu.VMEM((NBUF, d_model, COLS), bf),
                pltpu.SemaphoreType.DMA((NBUF,)),
                pltpu.SemaphoreType.DMA((14,)),
                pltpu.SemaphoreType.DMA((14,)),
            ],
            compiler_params=pltpu.CompilerParams(collective_id=0, has_side_effects=True, vmem_limit_bytes=67043328),
        )(x_loc, cos_t, sin_t, kc_loc.reshape(t, width), vc_loc.transpose(1, 2, 0).reshape(width, t), w_q, w_k, w_v, w_o)
        return y, k_new.reshape(t, heads, hd), v_new.reshape(t, heads, hd)

    return jax.shard_map(local_fn, mesh=mesh, in_specs=(row_spec, row_spec, row_spec, P(), P(), P(), P()), out_specs=(row_spec, row_spec, row_spec), check_vma=False)
```

```python
import functools
import math

import jax
import jax.numpy as jnp
from jax import lax
from jax.experimental import pallas as pl
from jax.experimental.pallas import tpu as pltpu
from jax.sharding import PartitionSpec as P

ROPE_BASE = 500000
MESH = pl.DeviceIdType.MESH
COLS = 512
NBUF = 6
QB = 512
SUB = 512
KB = 1024


def rope_tables(positions, head_dim):
    inv_freq = 1.0 / (ROPE_BASE ** (jnp.arange(0, head_dim, 2, dtype=jnp.float32) / head_dim))
    angles = positions.astype(jnp.float32)[:, None] * inv_freq[None, :]
    cos_t, sin_t = jnp.cos(angles), jnp.sin(angles)
    return jnp.concatenate([cos_t, cos_t], axis=-1), jnp.concatenate([-sin_t, sin_t], axis=-1)


def score_piece(i, q, k_at, s_buf, top, mask):
    s = lax.dot_general(k_at(i), q, (((1,), (1,)), ((), ())), preferred_element_type=jnp.float32)
    if mask is not None:
        s = jnp.where(mask(i), s, -jnp.inf)
    s_buf[i * SUB:(i + 1) * SUB, :] = s
    return jnp.maximum(top, jnp.max(s, axis=0, keepdims=True))


def online_step(s_buf, top, v_at, state, coef, pieces, ahead):
    m, l, acc = state
    m_new = jnp.maximum(m, top)
    alpha = jnp.exp2((m - m_new) * coef)
    l, acc = l * alpha, acc * alpha
    top_next = jnp.full_like(m, -jnp.inf)
    for i in range(pieces):
        top_next = score_piece(i, *ahead[:3], top_next, ahead[3])
        p = jnp.exp2((s_buf[i * SUB:(i + 1) * SUB, :] - m_new) * coef)
        l = l + jnp.sum(p.reshape(-1, 8, p.shape[1]), axis=0)
        acc = acc + jnp.dot(v_at(i), p.astype(jnp.bfloat16), preferred_element_type=jnp.float32)
    return (m_new, l, acc), top_next


def kernel(sp, cp, heads, head_dim,
           x_ref, cos_ref, sin_ref, kc_hbm, vc_hbm, wq_hbm, wk_hbm, wv_hbm, wo_hbm,
           y_ref, kn_ref, vn_ref,
           q_loc, vt_loc, q_all, kc_all, vc_all, kn_all, vn_all, o_all, o_loc,
           m_st, l_st, acc_st, s_a, s_b, s_c, wbuf, wsem, ssem, rsem):
    S = sp * cp
    E = heads - S
    G = S // E
    t = x_ref.shape[0]
    d_model = x_ref.shape[1]
    L = S * t
    me = lax.axis_index('sp') * cp + lax.axis_index('cp')
    per = S // (2 * G)
    rank = lax.rem(me, G)
    xhead = S + lax.div(me, G)
    my_blk = lax.div(me, per)
    my_rank = jnp.minimum(my_blk, 2 * G - 1 - my_blk)
    hi_share = my_blk >= G
    own_extra = my_rank == rank
    coef = (head_dim ** -0.5) * math.log2(math.e)

    X = cp // 2
    my_y, my_x, my_core = lax.div(me, cp), lax.div(lax.rem(me, cp), 2), lax.rem(me, 2)

    def peer(d):
        core, chip = lax.div(d, S // 2), lax.rem(d, S // 2)
        dx = lax.rem(chip, X)
        dy = lax.rem(lax.div(chip, X) + dx, sp)
        return lax.rem(my_y + dy, sp) * cp + lax.rem(my_x + dx, X) * 2 + lax.rem(my_core + core, 2)

    def dev(idx):
        return {'sp': lax.div(idx, cp), 'cp': lax.rem(idx, cp)}

    def col(h):
        return pl.ds(pl.multiple_of(h * head_dim, head_dim), head_dim)

    def rows(start, size):
        return pl.ds(pl.multiple_of(start, 128), size)

    def send(src, dst, sem, tgt):
        pltpu.make_async_remote_copy(src_ref=src, dst_ref=dst, send_sem=ssem.at[sem], recv_sem=rsem.at[sem],
                                     device_id=dev(tgt), device_id_type=MESH).start()

    def local(src, dst, sem):
        pltpu.make_async_copy(src, dst, rsem.at[sem]).start()

    def wait_recv(buf, sem):
        pltpu.make_async_copy(buf, buf, rsem.at[sem]).wait()

    def wait_sent(buf, n_pieces, sem):
        part = buf.at[pl.ds(0, n_pieces * t)]
        pltpu.make_async_copy(part, part, ssem.at[sem]).wait()

    tiles = d_model // COLS
    weights = (wq_hbm, wk_hbm, wv_hbm, wo_hbm)

    def fetch(w, tile, slot):
        return pltpu.make_async_copy(w.at[:, pl.ds(pl.multiple_of(tile * COLS, COLS), COLS)], wbuf.at[slot], wsem.at[slot])

    for tile in range(NBUF - 1):
        fetch(wq_hbm, tile, tile).start()

    barrier = pltpu.get_barrier_semaphore()

    def greet(d, carry):
        pl.semaphore_signal(barrier, inc=1, device_id=dev(lax.rem(me + d, S)), device_id_type=MESH)
        return carry

    lax.fori_loop(1, S, greet, 0)
    pl.semaphore_wait(barrier, S - 1)

    def head_of(sel, idx):
        return idx if sel == 0 else S + lax.div(idx, G)

    def k_piece(src, dst, sel, idx):
        return src.at[:, col(head_of(sel, idx))], dst.at[rows(sel * L + me * t, t)]

    def v_piece(src, dst, sel, idx):
        return (src.at[rows(head_of(sel, idx) * head_dim, head_dim)],
                dst.at[pl.ds(sel * head_dim, head_dim), rows(me * t, t)])

    def send_all(piece, src, dst, sem, sel):
        local(*piece(src, dst, sel, me), sem)

        def to_peer(d, carry):
            tgt = peer(d)
            send(*piece(src, dst, sel, tgt), sem, tgt)
            return carry

        lax.fori_loop(1, S if sel == 0 else S // 2, to_peer, 0)

    def pass_on(piece, dst, sem):
        def body(n, carry):
            region = piece(dst, dst, 1, 2 * n + my_core)
            send(region, region, sem, me + 1 - 2 * my_core)
            return carry

        lax.fori_loop(0, S // 2, body, 0)

    def k_region(_, dst, sel, idx):
        return dst.at[rows(sel * L + idx * t, t)]

    def v_region(_, dst, sel, idx):
        return dst.at[pl.ds(sel * head_dim, head_dim), rows(idx * t, t)]

    send_all(k_piece, kc_hbm, kc_all, 0, 0)
    send_all(v_piece, vc_hbm, vc_all, 1, 0)
    send_all(k_piece, kc_hbm, kc_all, 6, 1)
    send_all(v_piece, vc_hbm, vc_all, 7, 1)

    def project(which, out_fn, first_tile, next_w):
        def body(i, carry):
            step = which * tiles + i
            slot = lax.rem(step, NBUF)
            fetch(weights[which], i, slot).wait()
            acc = jnp.dot(out_fn[0][...], wbuf[slot], preferred_element_type=jnp.float32).astype(jnp.bfloat16)
            ahead = i + NBUF - 1
            nslot = lax.rem(step + NBUF - 1, NBUF)

            @pl.when(ahead < tiles)
            def _():
                fetch(weights[which], ahead, nslot).start()

            if next_w is not None:
                @pl.when(ahead >= tiles)
                def _():
                    fetch(next_w, ahead - tiles, nslot).start()

            out_fn[1](i, acc)
            return carry

        lax.fori_loop(first_tile, tiles, body, 0)

    def store_rope(dst):
        def put(i, val):
            for h in range(COLS // head_dim):
                piece = val[:, h * head_dim:(h + 1) * head_dim].astype(jnp.float32)
                turned = piece * cos_ref[...] + pltpu.roll(piece, head_dim // 2, 1) * sin_ref[...]
                dst[:, pl.ds(pl.multiple_of(i * COLS + h * head_dim, head_dim), head_dim)] = turned.astype(jnp.bfloat16)
        return put

    def store_plain(dst):
        def put(i, val):
            dst[:, pl.ds(pl.multiple_of(i * COLS, COLS), COLS)] = val
        return put

    def store_values(i, val):
        vn_ref[:, pl.ds(pl.multiple_of(i * COLS, COLS), COLS)] = val
        vt_loc[pl.ds(pl.multiple_of(i * COLS, COLS), COLS), :] = val.T

    project(0, (x_ref, store_rope(q_loc)), 0, wk_hbm)

    local(q_loc.at[:, col(me)], q_all.at[rows(me * t, t)], 2)

    def q_peer(d, carry):
        tgt = peer(d)
        send(q_loc.at[:, col(tgt)], q_all.at[rows(me * t, t)], 2, tgt)
        return carry

    lax.fori_loop(1, S, q_peer, 0)
    xrow = L + jnp.where(hi_share, per * t, 0) + lax.rem(me, per) * t

    def q_extra(g, carry):
        tgt = g * G + my_rank

        @pl.when(tgt == me)
        def _():
            local(q_loc.at[:, col(S + g)], q_all.at[rows(xrow, t)], 2)

        @pl.when(tgt != me)
        def _():
            send(q_loc.at[:, col(S + g)], q_all.at[rows(xrow, t)], 2, tgt)
        return carry

    lax.fori_loop(0, E, q_extra, 0)

    project(1, (x_ref, store_rope(kn_ref)), 0, wv_hbm)
    send_all(k_piece, kn_ref, kn_all, 3, 0)
    project(2, (x_ref, store_values), 0, wo_hbm)
    send_all(v_piece, vt_loc, vn_all, 4, 0)
    send_all(k_piece, kn_ref, kn_all, 8, 1)
    send_all(v_piece, vt_loc, vn_all, 9, 1)

    nmain = L // QB
    nq = nmain + 2 * per * t // QB

    def block_pos(qb):
        return jnp.where(qb < nmain, qb, jnp.where(qb == nmain, rank, 2 * G - 1 - rank))

    wait_recv(q_all, 2)
    main_part, half_part = kc_all.at[pl.ds(0, L)], kc_all.at[pl.ds(0, L // 2)]
    wait_recv(main_part, 0)
    wait_recv(main_part, 1)
    wait_recv(half_part, 6)
    wait_recv(half_part, 7)
    pass_on(k_region, kc_all, 10)
    pass_on(v_region, vc_all, 11)

    bufs = (s_a, s_b, s_c)

    def k_rows(buf, sel, start):
        return lambda i: buf[rows(sel * L + start + i * SUB, SUB), :]

    def v_cols(buf, sel, start):
        return lambda i: buf[rows(sel * head_dim, head_dim), rows(start + i * SUB, SUB)]

    def first_scores(q, k_at, s_buf, pieces):
        top = jnp.full((1, QB), -jnp.inf, jnp.float32)
        for i in range(pieces):
            top = score_piece(i, q, k_at, s_buf, top, None)
        return top

    def query(qb):
        return q_all[rows(qb * QB, QB), :]

    nst = L // KB

    def cache_block(sel, last, qb, top):
        after = jnp.minimum(qb + 1, last)
        q, q_after = query(qb), query(after)
        state = (jnp.full((1, QB), -jnp.inf, jnp.float32), jnp.zeros((8, QB), jnp.float32),
                 jnp.zeros((head_dim, QB), jnp.float32))
        for j in range(nst):
            if j + 1 < nst:
                ahead = (q, k_rows(kc_all, sel, (j + 1) * KB), bufs[(j + 1) % 2], None)
            else:
                ahead = (q_after, k_rows(kc_all, sel, 0), bufs[0], None)
            state, top = online_step(bufs[j % 2], top, v_cols(vc_all, sel, j * KB), state, coef, KB // SUB, ahead)
        m_st[qb, 0:1, :], l_st[qb], acc_st[qb] = state
        return top

    def cache_part(sel, carry):
        @pl.when(sel == 1)
        def _():
            wait_recv(half_part, 10)
            wait_recv(half_part, 11)

        start, stop = sel * nmain, jnp.where(sel == 0, nmain, nq)
        lax.fori_loop(start, stop, functools.partial(cache_block, sel, stop - 1),
                      first_scores(query(start), k_rows(kc_all, sel, 0), s_a, KB // SUB))
        return carry

    lax.fori_loop(0, 2, cache_part, 0)

    wait_recv(main_part, 3)
    wait_recv(main_part, 4)

    def send_out(qb):
        head = jnp.where(qb < nmain, me, xhead)
        for piece in range(QB // t):
            tgt = block_pos(qb) * (QB // t) + piece
            src = o_all.at[rows(qb * QB + piece * t, t)]
            dst = o_loc.at[:, col(head)]

            @pl.when(tgt == me)
            def _():
                local(src, dst, 5)

            @pl.when(tgt != me)
            def _():
                send(src, dst, 5, tgt)

    nfull = nmain - 1

    def item(i, n):
        qa = jnp.where(i < nmain // 2, i, nmain)
        qb = jnp.where(i < nmain // 2, nmain - 1 - i, nmain + 1)
        pa, pb = block_pos(qa), block_pos(qb)
        if n < nfull:
            early = n < pa
            return jnp.where(early, qa, qb), jnp.where(early, n, n - pa), None
        blk, pos = (qa, pa) if n == nfull else (qb, pb)
        return blk, pos, lambda piece: (lax.broadcasted_iota(jnp.int32, (SUB, QB), 0) + piece * SUB
                                        <= lax.broadcasted_iota(jnp.int32, (SUB, QB), 1))

    def new_pair(sel, last, i, top):
        after = jnp.minimum(i + 1, last)

        @pl.when(i == nmain // 2 - 1)
        def _():
            wait_recv(half_part, 8)
            wait_recv(half_part, 9)
            pass_on(k_region, kn_all, 12)
            pass_on(v_region, vn_all, 13)

        for n in range(nfull + 2):
            blk, pos, _ = item(i, n)
            nblk, npos, nmask = item(i, n + 1) if n + 1 < nfull + 2 else item(after, 0)
            ahead = (query(nblk), k_rows(kn_all, sel, npos * QB), bufs[(n + 1) % 3], nmask)
            state = (m_st[blk, 0:1, :], l_st[blk], acc_st[blk])
            state, top = online_step(bufs[n % 3], top, v_cols(vn_all, sel, pos * QB), state, coef,
                                     QB // SUB, ahead)
            if n < nfull:
                m_st[blk, 0:1, :], l_st[blk], acc_st[blk] = state
            else:
                out = (state[2] / jnp.sum(state[1], axis=0, keepdims=True)).astype(jnp.bfloat16)
                o_all[rows(blk * QB, QB), :] = out.T

        send_out(item(i, nfull)[0])
        send_out(item(i, nfull + 1)[0])
        return top

    def new_part(sel, carry):
        @pl.when(sel == 1)
        def _():
            wait_recv(half_part, 12)
            wait_recv(half_part, 13)

        start, stop = sel * (nmain // 2), jnp.where(sel == 0, nmain // 2, nq // 2)
        blk0, pos0, _ = item(start, 0)
        lax.fori_loop(start, stop, functools.partial(new_pair, sel, stop - 1),
                      first_scores(query(blk0), k_rows(kn_all, sel, pos0 * QB), s_a, QB // SUB))
        return carry

    lax.fori_loop(0, 2, new_part, 0)

    wait_recv(o_loc, 5)
    project(3, (o_loc, store_plain(y_ref)), 0, None)

    for sem in (0, 1, 3, 4):
        wait_sent(kc_all, S - 1, sem)
    for sem in (6, 7, 8, 9):
        wait_sent(kc_all, S // 2 - 1, sem)
    for sem in (10, 11, 12, 13):
        wait_sent(kc_all, S // 2, sem)
    for sem in (2, 5):
        wait_sent(q_all, S - 1, sem)

        @pl.when(own_extra)
        def _():
            wait_sent(q_all, E - 1, sem)

        @pl.when(jnp.logical_not(own_extra))
        def _():
            wait_sent(q_all, E, sem)


def solution(mesh):
    sp, cp = mesh.shape['sp'], mesh.shape['cp']
    S = sp * cp
    row_spec = P(('dp', 'sp', 'cp'))

    def local_fn(x_loc, kc_loc, vc_loc, w_q, w_k, w_v, w_o):
        t, d_model = x_loc.shape
        _, heads, hd = kc_loc.shape
        G = S // (heads - S)
        L, X = S * t, S * t // G
        width = heads * hd
        chains = (L + X) // QB
        seq_idx = lax.axis_index('sp') * cp + lax.axis_index('cp')
        cos_t, sin_t = rope_tables(L + seq_idx * t + jnp.arange(t), hd)
        bf, f32 = jnp.bfloat16, jnp.float32
        vmem, hbm = pl.BlockSpec(memory_space=pltpu.VMEM), pl.BlockSpec(memory_space=pl.ANY)
        y, k_new, v_new = pl.pallas_call(
            functools.partial(kernel, sp, cp, heads, hd),
            out_shape=[jax.ShapeDtypeStruct((t, d_model), bf), jax.ShapeDtypeStruct((t, width), bf),
                       jax.ShapeDtypeStruct((t, width), bf)],
            in_specs=[vmem, vmem, vmem] + [hbm] * 6,
            out_specs=[vmem] * 3,
            scratch_shapes=[
                pltpu.VMEM((t, width), bf), pltpu.VMEM((width, t), bf),
                pltpu.VMEM((L + X, hd), bf),
                pltpu.VMEM((2 * L, hd), bf), pltpu.VMEM((2 * hd, L), bf),
                pltpu.VMEM((2 * L, hd), bf), pltpu.VMEM((2 * hd, L), bf),
                pltpu.VMEM((L + X, hd), bf),
                pltpu.VMEM((t, width), bf),
                pltpu.VMEM((chains, 8, QB), f32), pltpu.VMEM((chains, 8, QB), f32), pltpu.VMEM((chains, hd, QB), f32),
                pltpu.VMEM((KB, QB), f32), pltpu.VMEM((KB, QB), f32), pltpu.VMEM((QB, QB), f32),
                pltpu.VMEM((NBUF, d_model, COLS), bf),
                pltpu.SemaphoreType.DMA((NBUF,)),
                pltpu.SemaphoreType.DMA((14,)),
                pltpu.SemaphoreType.DMA((14,)),
            ],
            compiler_params=pltpu.CompilerParams(collective_id=0, has_side_effects=True, vmem_limit_bytes=67043328),
        )(x_loc, cos_t, sin_t, kc_loc.reshape(t, width), vc_loc.transpose(1, 2, 0).reshape(width, t), w_q, w_k, w_v, w_o)
        return y, k_new.reshape(t, heads, hd), v_new.reshape(t, heads, hd)

    return jax.shard_map(local_fn, mesh=mesh, in_specs=(row_spec, row_spec, row_spec, P(), P(), P(), P()), out_specs=(row_spec, row_spec, row_spec), check_vma=False)
```
